128 devices in a mesh: row: 16 (over y_hi, z, core), col: 8 (over y_lo, x).
Axes of the slice: x: 4, y: 4 (y_hi: 2, y_lo: 2; y = y_hi * 2 + y_lo), z: 4, core: 2. Of those that a mesh axis runs over, the one named last changes fastest.
Arguments:
- gate_input: bfloat16 [2, 1024, 53248], P(None, 'col', 'row'), may hold values from -6 to 6
- up_input: bfloat16 [2, 1024, 53248], P(None, 'col', 'row'), may hold values from -6 to 6
- down_weight: bfloat16 [53248, 16384], P('row', 'col'), may hold values from -0.02734375 to 0.02734375
Outputs:
- mixed: bfloat16 [2, 1024, 16384], P(None, 'row', 'col')
The draws below stay inside these ranges and needn't reach their ends.
All inputs are finite; a program needn't handle non-finite values.
Results may differ from the reference program's by a relative error of at most 0.0049.
Values may be sent and summed in bfloat16 or wider, within the bound.
A program may use at most 128 MiB of HBM per device.

```python
import jax
import jax.numpy as jnp

D = 16384
FF = 53248
SEQS = 2
MINISEQ = 1024


def block_scale(key, dims, cuts, least, top_value):
    loudness = 1.0
    for axis_at, blocks in cuts:
        steps = jax.random.uniform(jax.random.fold_in(jax.random.fold_in(key, 6), axis_at), (blocks,), jnp.float32, least / len(cuts), top_value / len(cuts))
        loudness = loudness * jnp.repeat(jnp.exp(steps), dims[axis_at] // blocks).reshape((-1,) + (1,) * (len(dims) - 1 - axis_at))
    return loudness


def centred(own_key, shape, width, most, split=(), dtype=jnp.bfloat16):
    values = width * jax.random.normal(own_key, shape, jnp.float32)
    if split:
        values = values * block_scale(own_key, shape, split, -0.22, 0.18)
    return jnp.clip(values, -most, most).astype(dtype)


def setup_inputs(seed: int = 0) -> dict:
    key_of = jax.random.split(jax.random.key(seed), 4)
    gate_input = centred(key_of[0], (SEQS, MINISEQ, FF), 1.0, 6.0, ((1, 8), (2, 16)))
    up_input = centred(key_of[1], (SEQS, MINISEQ, FF), 1.0, 6.0, ((1, 8), (2, 16)))
    down_weight = centred(key_of[2], (FF, D), FF ** -0.5, 0.02734375, ((0, 16), (1, 8)))
    return dict(gate_input=gate_input, up_input=up_input, down_weight=down_weight)


def reference(gate_input, up_input, down_weight):
    hidden = (jax.nn.silu(gate_input.astype(jnp.float32)) * up_input.astype(jnp.float32)).astype(jnp.bfloat16)
    flat = hidden.reshape(SEQS * MINISEQ, FF)
    mixed = jnp.dot(flat, down_weight, preferred_element_type=jnp.float32)
    return mixed.astype(jnp.bfloat16).reshape(SEQS, MINISEQ, D)
```

```python
import functools

import jax
import jax.numpy as jnp
from jax import lax
from jax.experimental import pallas as pl
from jax.experimental.pallas import tpu as pltpu
from jax.sharding import PartitionSpec as P

MESH = pl.DeviceIdType.MESH

BLOCKS = 8
ROWS = 16
AHEAD = 3
GROUP_SIZES = (8, 8, 8, 8, 8, 8, 4, 4, 4, 4)

PLUS = (
    [(0, 0, 0), (0, 0, 1), (0, 0, 2), (3, 0, 0), (0, 1, 3), (3, 0, 2), (0, 1, 4), (0, 1, 5), (0, 1, 6), (0, 1, 7)]
    + [(0, 0, 3), (0, 0, 4), (3, 1, 3), (0, 0, 5), (3, 1, 5), (0, 0, 6), (3, 0, 4), (0, 0, 7), (3, 1, 7, 0), (3, 0, 6)]
)
MINUS = (
    [(0, 0, 1), (0, 0, 0), (0, 0, 2), (1, 0, 1), (0, 1, 3), (0, 1, 4), (0, 1, 5), (0, 1, 6), (0, 1, 7), (0, 0, 3)]
    + [(0, 0, 4), (1, 1, 4), (0, 0, 5), (1, 1, 6), (1, 0, 3), (0, 0, 6), (0, 0, 7), (1, 0, 5), (1, 1, 7, 1), (1, 0, 7)]
)
ACROSS = (
    [(0, 0, 3), (0, 0, 4), (0, 0, 5), (0, 0, 6), (0, 0, 7), (0, 0, 0), (0, 0, 1), (0, 0, 2)]
    + [(3, 0, 0), (1, 0, 0), (3, 0, 1), (1, 0, 1), (3, 0, 2), (1, 0, 2), (2, 0, 0), (2, 0, 1), (2, 0, 2)]
)
OWN_ORDER = (0, 3, 1, 4, 2, 5, 6, 7)


def plan():
    links = []
    for items, shift_x, shift_y in ((PLUS, 3, 0), (MINUS, 1, 0), (ACROSS, 0, 1)):
        link = []
        for item in items:
            dx, dy, block = item[:3]
            half = item[3] if len(item) > 3 else None
            link.append(((dx, dy, block), half, ((dx + shift_x) % 4, dy ^ shift_y, block)))
        links.append(link)
    order = [(0, 0, b) for b in range(BLOCKS)]
    arrived_at = {key: -1 for key in order}
    slots = max(len(link) for link in links)
    for slot in range(slots):
        for link in links:
            if slot < len(link):
                key = link[slot][2]
                if key not in arrived_at:
                    order.append(key)
                arrived_at[key] = slot
    assert len(order) == 8 * BLOCKS
    for link in links:
        for slot, (source, _, _) in enumerate(link):
            assert arrived_at[source] <= slot - AHEAD or arrived_at[source] == -1
    groups, at = [], 0
    for size in GROUP_SIZES:
        groups.append(order[at : at + size])
        at += size
    assert at == len(order)
    place = {key: (g, q) for g, group in enumerate(groups) for q, key in enumerate(group)}
    start = [sum(GROUP_SIZES[:g]) for g in range(len(GROUP_SIZES))]
    ready = [max(arrived_at[key] for key in group) for group in groups]
    return links, groups, place, start, ready, slots


LINKS, GROUPS, PLACE, START, READY, SLOTS = plan()
N_GROUPS = len(GROUPS)
TILE_N = 512


def kernel(gate_ref, up_ref, weight_ref, out_ref, *scratch):
    hidden = scratch[:N_GROUPS]
    (gate_buf, up_buf, weight, result, halves, z_out, z_in, y_out, y_in) = scratch[N_GROUPS : N_GROUPS + 9]
    (load_sem, weight_sem, send_sem, recv_sem, pair_send, pair_recv, z_send, z_recv, y_send, y_recv) = scratch[N_GROUPS + 9 :]
    row = lax.axis_index("row")
    col = lax.axis_index("col")
    y_hi, z, core = row // 8, (row // 2) % 4, row % 2
    y_lo, x = col // 4, col % 4
    across = (row, (1 - y_lo) * 4 + x)
    plus = (row, y_lo * 4 + (x + 1) % 4)
    minus = (row, y_lo * 4 + (x + 3) % 4)
    partner = (y_hi * 8 + z * 2 + (1 - core), col)
    far = ((1 - y_hi) * 8 + z * 2 + core, col)
    targets = (plus, minus, across)
    root_dx = (z + 4 - x) % 4
    final_dy = (y_hi + y_lo) % 2

    def z_device(other):
        return (y_hi * 8 + other * 2 + core, col)

    barrier = pltpu.get_barrier_semaphore()
    for device in (plus, minus, across, partner, far, z_device((z + 1) % 4), z_device((z + 2) % 4), z_device((z + 3) % 4)):
        pl.semaphore_signal(barrier, inc=1, device_id=device, device_id_type=MESH)

    def load(block):
        s, j = divmod(block, 4)
        rows = pl.ds(j * ROWS, ROWS)
        return (
            pltpu.make_async_copy(gate_ref.at[s, :, rows, :], gate_buf.at[block], load_sem.at[0, block]),
            pltpu.make_async_copy(up_ref.at[s, :, rows, :], up_buf.at[block], load_sem.at[1, block]),
        )

    for block in OWN_ORDER:
        for copy in load(block):
            copy.start()
    weight_copy = pltpu.make_async_copy(weight_ref, weight, weight_sem)
    weight_copy.start()

    def view(key, half):
        g, q = PLACE[key]
        return hidden[g].at[:, q] if half is None else hidden[g].at[half, q]

    def transfer(link, slot):
        source, half, target = LINKS[link][slot]
        return pltpu.make_async_remote_copy(
            src_ref=view(source, half),
            dst_ref=view(target, half),
            send_sem=send_sem.at[link, slot],
            recv_sem=recv_sem.at[link, slot],
            device_id=targets[link],
            device_id_type=MESH,
        )

    greeted = False
    pending = [(link, slot) for slot in range(AHEAD) for link in range(3)]
    done = set()
    for block in OWN_ORDER:
        for copy in load(block):
            copy.wait()

        def gate_half(h, carry, block=block):
            gate = gate_buf[block, h].astype(jnp.float32)
            up = up_buf[block, h].astype(jnp.float32)
            hidden[0][h, block] = ((0.5 * gate) * (1.0 + jnp.tanh(0.5 * gate)) * up).astype(jnp.bfloat16)
            return carry

        lax.fori_loop(0, 2, gate_half, 0)
        if not greeted:
            pl.semaphore_wait(barrier, 8)
            greeted = True
        done.add(block)
        for link, slot in list(pending):
            if LINKS[link][slot][0][2] in done and not any(l == link and s < slot for l, s in pending):
                transfer(link, slot).start()
                pending.remove((link, slot))
    assert not pending
    weight_copy.wait()

    def pair_copy(g):
        size = GROUP_SIZES[g]
        return pltpu.make_async_remote_copy(
            src_ref=result.at[g % 2, 1 - core, pl.ds(0, size)],
            dst_ref=halves.at[pl.ds(START[g], size)],
            send_sem=pair_send.at[g],
            recv_sem=pair_recv.at[g],
            device_id=partner,
            device_id_type=MESH,
        )

    def z_copy(g, q):
        dx, dy, block = GROUPS[g][q]
        root = (x + dx) % 4
        offset = (z + 4 - root) % 4 - 1
        return root, pltpu.make_async_remote_copy(
            src_ref=z_out.at[START[g] + q],
            dst_ref=z_in.at[dy * BLOCKS + block, offset],
            send_sem=z_send.at[START[g] + q],
            recv_sem=z_recv.at[dy * BLOCKS + block, offset],
            device_id=z_device(root),
            device_id_type=MESH,
        )

    def z_arrival(dy, block, offset):
        return pltpu.make_async_remote_copy(
            src_ref=z_in.at[dy * BLOCKS + block, offset],
            dst_ref=z_in.at[dy * BLOCKS + block, offset],
            send_sem=z_send.at[0],
            recv_sem=z_recv.at[dy * BLOCKS + block, offset],
            device_id=z_device((z + 1) % 4),
            device_id_type=MESH,
        )

    def y_copy(dy, block):
        return pltpu.make_async_remote_copy(
            src_ref=y_out.at[dy * BLOCKS + block],
            dst_ref=y_in.at[block],
            send_sem=y_send.at[dy * BLOCKS + block],
            recv_sem=y_recv.at[block],
            device_id=far,
            device_id_type=MESH,
        )

    def multiply(g):
        size = GROUP_SIZES[g]
        if g >= 2:
            pair_copy(g - 2).wait_send()

        def tile(n, carry):
            columns = pl.ds(pl.multiple_of(n * TILE_N, TILE_N), TILE_N)
            left = hidden[g][...].reshape(size * 2 * ROWS, -1)
            value = jnp.dot(left, weight[:, columns], preferred_element_type=jnp.float32)
            result[g % 2, :, pl.ds(0, size), :, columns] = value.reshape(2, size, ROWS, TILE_N)
            return carry

        lax.fori_loop(0, weight.shape[1] // TILE_N, tile, 0)
        pair_copy(g).start()

    def add_pair(g):
        pair_copy(g).wait_recv()

        def one(q, carry):
            at = START[g] + q
            value = halves[at] + result[g % 2, core, q]
            halves[at] = value
            z_out[at] = value.astype(jnp.bfloat16)
            return carry

        lax.fori_loop(0, GROUP_SIZES[g], one, 0)
        for q in range(GROUP_SIZES[g]):
            root, copy = z_copy(g, q)

            @pl.when(root != z)
            def _():
                copy.start()

    def add_z(g):
        for q, (dx, dy, block) in enumerate(GROUPS[g]):
            at = START[g] + q

            @pl.when(root_dx == dx)
            def _():
                for offset in range(3):
                    z_arrival(dy, block, offset).wait_recv()

                def tile(n, carry):
                    columns = pl.ds(pl.multiple_of(n * TILE_N, TILE_N), TILE_N)
                    value = halves[at, :, columns]
                    for offset in range(3):
                        value = value + z_in[dy * BLOCKS + block, offset, :, columns].astype(jnp.float32)
                    halves[at, :, columns] = value
                    y_out[dy * BLOCKS + block, :, columns] = value.astype(jnp.bfloat16)
                    return carry

                lax.fori_loop(0, weight.shape[1] // TILE_N, tile, 0)

                @pl.when(final_dy != dy)
                def _():
                    y_copy(dy, block).start()

    def add_y(g):
        for q, (dx, dy, block) in enumerate(GROUPS[g]):
            at = START[g] + q
            s, j = divmod(block, 4)

            @pl.when((root_dx == dx) & (final_dy == dy))
            def _():
                y_copy(dy, block).wait_recv()

                def tile(n, carry):
                    columns = pl.ds(pl.multiple_of(n * TILE_N, TILE_N), TILE_N)
                    value = halves[at, :, columns] + y_in[block, :, columns].astype(jnp.float32)
                    out_ref[s, pl.ds(j * ROWS, ROWS), columns] = value.astype(jnp.bfloat16)
                    return carry

                lax.fori_loop(0, weight.shape[1] // TILE_N, tile, 0)

    def step(g):
        multiply(g)
        if g >= 1:
            add_pair(g - 1)
        if g >= 3:
            add_z(g - 3)
        if g >= 5:
            add_y(g - 5)

    step(0)
    for slot in range(SLOTS):
        for link in range(3):
            if slot < len(LINKS[link]):
                transfer(link, slot).wait_recv()
        for link in range(3):
            if slot + AHEAD < len(LINKS[link]):
                transfer(link, slot + AHEAD).start()
        for g in range(1, N_GROUPS):
            if READY[g] == slot:
                step(g)
    last = N_GROUPS - 1
    add_z(last - 2)
    add_pair(last)
    add_y(last - 4)
    add_z(last - 1)
    add_y(last - 3)
    add_z(last)
    for g in range(last - 2, last + 1):
        add_y(g)

    for link in range(3):
        for slot in range(len(LINKS[link])):
            transfer(link, slot).wait_send()
    pair_copy(last - 1).wait_send()
    pair_copy(last).wait_send()
    for g in range(N_GROUPS):
        for q in range(GROUP_SIZES[g]):
            root, copy = z_copy(g, q)

            @pl.when(root != z)
            def _():
                copy.wait_send()

    for dy in range(2):
        for block in range(BLOCKS):

            @pl.when(final_dy != dy)
            def _():
                y_copy(dy, block).wait_send()


def body(gate_input, up_input, down_weight):
    seqs, tokens, units = gate_input.shape
    width = down_weight.shape[1]
    halved = (seqs, 2, tokens // 2, units)
    bf16, f32 = jnp.bfloat16, jnp.float32
    dma = pltpu.SemaphoreType.DMA
    any_spec = pl.BlockSpec(memory_space=pl.ANY)
    return pl.pallas_call(
        kernel,
        out_shape=jax.ShapeDtypeStruct((seqs, tokens // 2, width), bf16),
        in_specs=[any_spec, any_spec, any_spec],
        out_specs=pl.BlockSpec(memory_space=pltpu.VMEM),
        scratch_shapes=[
            *[pltpu.VMEM((2, size, ROWS, units), bf16) for size in GROUP_SIZES],
            pltpu.VMEM((BLOCKS, 2, ROWS, units), bf16),
            pltpu.VMEM((BLOCKS, 2, ROWS, units), bf16),
            pltpu.VMEM((units, width), bf16),
            pltpu.VMEM((2, 2, BLOCKS, ROWS, width), f32),
            pltpu.VMEM((8 * BLOCKS, ROWS, width), f32),
            pltpu.VMEM((8 * BLOCKS, ROWS, width), bf16),
            pltpu.VMEM((2 * BLOCKS, 3, ROWS, width), bf16),
            pltpu.VMEM((2 * BLOCKS, ROWS, width), bf16),
            pltpu.VMEM((BLOCKS, ROWS, width), bf16),
            dma((2, BLOCKS)),
            dma,
            dma((3, SLOTS)),
            dma((3, SLOTS)),
            dma((N_GROUPS,)),
            dma((N_GROUPS,)),
            dma((8 * BLOCKS,)),
            dma((2 * BLOCKS, 3)),
            dma((2 * BLOCKS,)),
            dma((BLOCKS,)),
        ],
        compiler_params=pltpu.CompilerParams(
            collective_id=0, has_side_effects=True, vmem_limit_bytes=63 * 1024 * 1024
        ),
    )(gate_input.reshape(halved), up_input.reshape(halved), down_weight)


def solution(mesh):
    return jax.shard_map(
        body,
        mesh=mesh,
        in_specs=(P(None, "col", "row"), P(None, "col", "row"), P("row", "col")),
        out_specs=P(None, "row", "col"),
        check_vma=False,
    )
```

```python
import functools

import jax
import jax.numpy as jnp
from jax import lax
from jax.experimental import pallas as pl
from jax.experimental.pallas import tpu as pltpu
from jax.sharding import PartitionSpec as P

MESH = pl.DeviceIdType.MESH

BLOCKS = 8
ROWS = 16
AHEAD = 3
GROUP_SIZES = (8, 6, 6, 6, 6, 5, 6, 4, 6, 6, 2, 3)
LAST = len(GROUP_SIZES) - 1
PARTS = 2

PLUS = (
    [(0, 0, 0), (0, 0, 2), (0, 0, 1), (3, 0, 0), (0, 1, 3), (3, 0, 2), (0, 1, 5), (3, 1, 3), (0, 0, 4), (0, 1, 7)]
    + [(3, 1, 5), (3, 0, 4), (0, 0, 6), (3, 1, 7, 0), (0, 0, 3), (3, 0, 6), (0, 1, 4), (0, 0, 5), (0, 1, 6), (0, 0, 7)]
)
MINUS = (
    [(0, 0, 1), (0, 0, 0), (0, 0, 3), (1, 0, 1), (0, 1, 4), (1, 0, 3), (0, 1, 6), (1, 1, 4), (0, 0, 5), (0, 1, 7)]
    + [(1, 1, 6), (1, 0, 5), (0, 0, 7), (1, 1, 7, 1), (0, 0, 2), (1, 0, 7), (0, 1, 3), (0, 0, 4), (0, 1, 5), (0, 0, 6)]
)
ACROSS = (
    [(0, 0, 3), (0, 0, 4), (0, 0, 5), (0, 0, 6), (0, 0, 7), (3, 0, 0), (1, 0, 1), (2, 0, 0), (2, 0, 1), None]
    + [(1, 0, 0), (2, 0, 2), (3, 0, 2), None, (3, 0, 1), (0, 0, 0), (0, 0, 1), (1, 0, 2), None, (0, 0, 2)]
)
OWN_ORDER = (0, 1, 3, 2, 4, 5, 6, 7)


def plan():
    links = []
    for items, shift_x, shift_y in ((PLUS, 3, 0), (MINUS, 1, 0), (ACROSS, 0, 1)):
        link = []
        for item in items:
            if item is None:
                link.append(None)
                continue
            dx, dy, block = item[:3]
            half = item[3] if len(item) > 3 else None
            link.append(((dx, dy, block), half, ((dx + shift_x) % 4, dy ^ shift_y, block)))
        links.append(link)
    order = [(0, 0, b) for b in range(BLOCKS)]
    arrived_at = {key: -1 for key in order}
    slots = max(len(link) for link in links)
    for slot in range(slots):
        for link in links:
            if slot < len(link) and link[slot]:
                key = link[slot][2]
                if key not in arrived_at:
                    order.append(key)
                arrived_at[key] = slot
    assert len(order) == 8 * BLOCKS
    issue = {}
    for link in links:
        for slot, item in enumerate(link):
            source = item[0] if item else order[0]
            issue.setdefault(max(arrived_at[source], slot - AHEAD, -1), []).append((links.index(link), slot))
    groups, at = [], 0
    for size in GROUP_SIZES:
        groups.append(sorted(order[at : at + size]))
        at += size
    assert at == len(order)
    place = {key: (g, q) for g, group in enumerate(groups) for q, key in enumerate(group)}
    start = [sum(GROUP_SIZES[:g]) for g in range(len(GROUP_SIZES))]
    ready = [max(arrived_at[key] for key in group) for group in groups]
    return links, groups, place, start, ready, slots, issue


LINKS, GROUPS, PLACE, START, READY, SLOTS, ISSUE = plan()
N_GROUPS = len(GROUPS)
UNITS = [(g, 0) for g in range(LAST)] + [(LAST, part) for part in range(PARTS)]
TILE_N = 512


def runs_of(g):
    runs = []
    for dx in range(4):
        places = [q for q, key in enumerate(GROUPS[g]) if key[0] == dx]
        if places:
            rank = sum(key[0] == dx for group in GROUPS[:g] for key in group)
            runs.append((dx, places[0], len(places), rank))
    return runs


def y_runs_of(g, dx):
    runs = []
    for dy in range(2):
        places = [q for q, key in enumerate(GROUPS[g]) if key[:2] == (dx, dy)]
        if places:
            rank = sum(key[:2] == (dx, dy) for group in GROUPS[:g] for key in group)
            runs.append((dy, places[0], len(places), rank))
    return runs


def kernel(gate_ref, up_ref, weight_ref, out_ref, *scratch):
    hidden = scratch[:N_GROUPS]
    (gate_buf, up_buf, weight, result, halves, z_out, z_in, y_out, y_in) = scratch[N_GROUPS : N_GROUPS + 9]
    last_bufs = scratch[N_GROUPS + 9 : N_GROUPS + 15]
    (load_sem, weight_sem, send_sem, recv_sem, pair_send, pair_recv, z_send, z_recv, y_send, y_recv) = scratch[N_GROUPS + 15 :]
    result_last, halves_last, z_out_last, z_in_last, y_out_last, y_in_last = last_bufs
    row = lax.axis_index("row")
    col = lax.axis_index("col")
    y_hi, z, core = row // 8, (row // 2) % 4, row % 2
    y_lo, x = col // 4, col % 4
    across = (row, (1 - y_lo) * 4 + x)
    plus = (row, y_lo * 4 + (x + 1) % 4)
    minus = (row, y_lo * 4 + (x + 3) % 4)
    partner = (y_hi * 8 + z * 2 + (1 - core), col)
    far = ((1 - y_hi) * 8 + z * 2 + core, col)
    targets = (plus, minus, across)
    root_dx = (z + 4 - x) % 4
    final_dy = (y_hi + y_lo) % 2

    def z_device(other):
        return (y_hi * 8 + other * 2 + core, col)

    barrier = pltpu.get_barrier_semaphore()
    for device in (plus, minus, across, partner, far, z_device((z + 1) % 4), z_device((z + 2) % 4), z_device((z + 3) % 4)):
        pl.semaphore_signal(barrier, inc=1, device_id=device, device_id_type=MESH)

    def load(block):
        s, j = divmod(block, 4)
        rows = pl.ds(j * ROWS, ROWS)
        return (
            pltpu.make_async_copy(gate_ref.at[s, :, rows, :], gate_buf.at[block], load_sem.at[0, block]),
            pltpu.make_async_copy(up_ref.at[s, :, rows, :], up_buf.at[block], load_sem.at[1, block]),
        )

    for block in OWN_ORDER:
        for copy in load(block):
            copy.start()
    weight_copy = pltpu.make_async_copy(weight_ref, weight, weight_sem)
    weight_copy.start()

    def view(key, half):
        g, q = PLACE[key]
        return hidden[g].at[q] if half is None else hidden[g].at[q, half]

    def transfer(link, slot):
        source, half, target = LINKS[link][slot]
        return pltpu.make_async_remote_copy(
            src_ref=view(source, half),
            dst_ref=view(target, half),
            send_sem=send_sem.at[link, slot],
            recv_sem=recv_sem.at[link, slot],
            device_id=targets[link],
            device_id_type=MESH,
        )

    greeted = False
    pending = sorted((i for i in ISSUE[-1] if LINKS[i[0]][i[1]]), key=lambda i: i[1])
    done = set()
    for block in OWN_ORDER:
        for copy in load(block):
            copy.wait()

        def gate_half(h, carry, block=block):
            gate = gate_buf[block, h].astype(jnp.float32)
            up = up_buf[block, h].astype(jnp.float32)
            hidden[0][block, h] = ((0.5 * gate) * (1.0 + jnp.tanh(0.5 * gate)) * up).astype(jnp.bfloat16)
            return carry

        lax.fori_loop(0, 2, gate_half, 0)
        if not greeted:
            pl.semaphore_wait(barrier, 8)
            greeted = True
        done.add(block)
        for link, slot in list(pending):
            if LINKS[link][slot][0][2] in done and not any(l == link and s < slot for l, s in pending):
                transfer(link, slot).start()
                pending.remove((link, slot))
    assert not pending
    weight_copy.wait()
    width = weight.shape[1]

    def sums(g, part):
        return halves_last.at[part] if g == LAST else halves.at[pl.ds(START[g], GROUP_SIZES[g])]

    def outgoing(g, part):
        return z_out_last.at[part] if g == LAST else z_out.at[pl.ds(START[g], GROUP_SIZES[g])]

    def products(g, part, half):
        return result_last.at[part, half] if g == LAST else result.at[g % 2, half, pl.ds(0, GROUP_SIZES[g])]

    def z_landing(g, part, offset, run):
        _, first, count, rank = run
        return z_in_last.at[part, offset, pl.ds(first, count)] if g == LAST else z_in.at[offset, pl.ds(rank, count)]

    def y_leaving(g, part, run, y_run):
        _, z_first, _, rank = run
        _, first, count, _ = y_run
        if g == LAST:
            return y_out_last.at[part, pl.ds(first, count)]
        return y_out.at[pl.ds(rank + first - z_first, count)]

    def y_landing(g, part, y_run):
        _, first, count, rank = y_run
        return y_in_last.at[part, pl.ds(first, count)] if g == LAST else y_in.at[pl.ds(rank, count)]

    def remote(source, target, sent, received, device):
        return pltpu.make_async_remote_copy(
            src_ref=source, dst_ref=target, send_sem=sent, recv_sem=received, device_id=device, device_id_type=MESH
        )

    def pair_copy(g, part):
        unit = g + part
        return remote(products(g, part, 1 - core), sums(g, part), pair_send.at[unit], pair_recv.at[unit], partner)

    def z_copy(g, part, run):
        dx, first, count, _ = run
        root = (x + dx) % 4
        offset = (z + 4 - root) % 4 - 1
        unit = g + part
        source = outgoing(g, part).at[pl.ds(first, count)]
        return root, remote(
            source, z_landing(g, part, offset, run), z_send.at[unit, dx], z_recv.at[unit, offset], z_device(root)
        )

    def z_arrival(g, part, offset, run):
        landed = z_landing(g, part, offset, run)
        return remote(landed, landed, z_send.at[0, 0], z_recv.at[g + part, offset], z_device((z + 1) % 4))

    def y_copy(g, part, run, y_run):
        unit = g + part
        return remote(y_leaving(g, part, run, y_run), y_landing(g, part, y_run), y_send.at[unit], y_recv.at[unit], far)

    def multiply(g, part):
        size = GROUP_SIZES[g]
        span = width // PARTS if g == LAST else width

        def tile(n, carry):
            columns = pl.ds(pl.multiple_of(n * TILE_N, TILE_N), TILE_N)
            taken = pl.ds(pl.multiple_of(n * TILE_N + part * span, TILE_N), TILE_N)
            left = hidden[g][...].reshape(size * 2 * ROWS, -1)
            value = jnp.dot(left, weight[:, taken], preferred_element_type=jnp.float32)
            value = value.reshape(size, 2, ROWS, TILE_N)
            for half in range(2):
                products(g, part, half)[:, :, columns] = value[:, half]
            return carry

        lax.fori_loop(0, span // TILE_N, tile, 0)
        pair_copy(g, part).start()

    def tiles(count, span, body):
        steps = span // TILE_N

        def one(i, carry):
            body(i // steps, pl.ds(pl.multiple_of(i % steps * TILE_N, TILE_N), TILE_N))
            return carry

        lax.fori_loop(0, count * steps, one, 0)

    def add_pair(g, part):
        pair_copy(g, part).wait_recv()
        own, total, out = products(g, part, core), sums(g, part), outgoing(g, part)

        def add(q, columns):
            value = total[q, :, columns] + own[q, :, columns]
            total[q, :, columns] = value
            out[q, :, columns] = value.astype(jnp.bfloat16)

        tiles(GROUP_SIZES[g], total.shape[-1], add)
        for run in runs_of(g):
            root, copy = z_copy(g, part, run)

            @pl.when(root != z)
            def _():
                copy.start()

        pair_copy(g, part).wait_send()

    def add_z(g, part=0):
        for run in runs_of(g):
            dx, first, count, _ = run

            @pl.when(root_dx == dx)
            def _():
                total = sums(g, part)
                for offset in range(3):
                    z_arrival(g, part, offset, run).wait_recv()
                for y_run in y_runs_of(g, dx):
                    dy, y_first, y_count, _ = y_run
                    leaving = y_leaving(g, part, run, y_run)

                    def add(q, columns):
                        value = total[y_first + q, :, columns]
                        for offset in range(3):
                            landed = z_landing(g, part, offset, run)
                            value = value + landed[y_first - first + q, :, columns].astype(jnp.float32)
                        total[y_first + q, :, columns] = value
                        leaving[q, :, columns] = value.astype(jnp.bfloat16)

                    tiles(y_count, total.shape[-1], add)

                    @pl.when(final_dy != dy)
                    def _():
                        y_copy(g, part, run, y_run).start()

    def add_y(g, part=0):
        for run in runs_of(g):
            dx = run[0]
            for y_run in y_runs_of(g, dx):
                dy, y_first, y_count, _ = y_run

                @pl.when((root_dx == dx) & (final_dy == dy))
                def _():
                    total, landed = sums(g, part), y_landing(g, part, y_run)
                    span = total.shape[-1]
                    y_copy(g, part, run, y_run).wait_recv()
                    for q in range(y_count):
                        s, j = divmod(GROUPS[g][y_first + q][2], 4)

                        def add(_, columns):
                            value = total[y_first + q, :, columns] + landed[q, :, columns].astype(jnp.float32)
                            taken = pl.ds(pl.multiple_of(columns.start + part * span, TILE_N), TILE_N)
                            out_ref[s, pl.ds(j * ROWS, ROWS), taken] = value.astype(jnp.bfloat16)

                        tiles(1, span, add)

    z_work = {4: (0, 1), 5: (2,), 6: (3,), 7: (4,), 8: (5,), 9: (6,), 10: (7,)}
    y_work = {7: (0, 1), 8: (2,), 9: (3,), 10: (4,)}

    def step(g):
        multiply(g, 0)
        for older in z_work.get(g, ()):
            add_z(older)
        for older in y_work.get(g, ()):
            add_y(older)
        add_pair(g, 0)

    def last_step():
        multiply(LAST, 0)
        add_z(LAST - 3)
        multiply(LAST, 1)
        add_pair(LAST, 0)
        add_pair(LAST, 1)
        add_y(LAST - 6)
        add_z(LAST - 2)
        add_z(LAST - 1)
        add_y(LAST - 5)
        add_z(LAST, 0)
        add_y(LAST - 4)
        add_z(LAST, 1)
        for g in range(LAST - 3, LAST):
            add_y(g)
        add_y(LAST, 0)
        add_y(LAST, 1)

    step(0)
    for slot in range(SLOTS):
        for link in range(3):
            if LINKS[link][slot]:
                transfer(link, slot).wait_recv()
        for link, later in sorted(ISSUE.get(slot, ()), key=lambda i: i[1]):
            if LINKS[link][later]:
                transfer(link, later).start()
        for g in range(1, N_GROUPS):
            if READY[g] == slot:
                step(g) if g < LAST else last_step()

    for link in range(3):
        for slot in range(SLOTS):
            if LINKS[link][slot]:
                transfer(link, slot).wait_send()
    for g, part in UNITS:
        for run in runs_of(g):
            root, copy = z_copy(g, part, run)

            @pl.when(root != z)
            def _():
                copy.wait_send()

            for y_run in y_runs_of(g, run[0]):

                @pl.when((root_dx == run[0]) & (final_dy != y_run[0]))
                def _():
                    y_copy(g, part, run, y_run).wait_send()


def body(gate_input, up_input, down_weight):
    seqs, tokens, units = gate_input.shape
    width = down_weight.shape[1]
    halved = (seqs, 2, tokens // 2, units)
    bf16, f32 = jnp.bfloat16, jnp.float32
    dma = pltpu.SemaphoreType.DMA
    last, part_width = GROUP_SIZES[LAST], width // PARTS
    earlier = 8 * BLOCKS - last
    any_spec = pl.BlockSpec(memory_space=pl.ANY)
    return pl.pallas_call(
        kernel,
        out_shape=jax.ShapeDtypeStruct((seqs, tokens // 2, width), bf16),
        in_specs=[any_spec, any_spec, any_spec],
        out_specs=pl.BlockSpec(memory_space=pltpu.VMEM),
        scratch_shapes=[
            *[pltpu.VMEM((size, 2, ROWS, units), bf16) for size in GROUP_SIZES],
            pltpu.VMEM((BLOCKS, 2, ROWS, units), bf16),
            pltpu.VMEM((BLOCKS, 2, ROWS, units), bf16),
            pltpu.VMEM((units, width), bf16),
            pltpu.VMEM((2, 2, BLOCKS, ROWS, width), f32),
            pltpu.VMEM((earlier, ROWS, width), f32),
            pltpu.VMEM((earlier, ROWS, width), bf16),
            pltpu.VMEM((3, 2 * BLOCKS, ROWS, width), bf16),
            pltpu.VMEM((2 * BLOCKS, ROWS, width), bf16),
            pltpu.VMEM((BLOCKS, ROWS, width), bf16),
            pltpu.VMEM((PARTS, 2, last, ROWS, part_width), f32),
            pltpu.VMEM((PARTS, last, ROWS, part_width), f32),
            pltpu.VMEM((PARTS, last, ROWS, part_width), bf16),
            pltpu.VMEM((PARTS, 3, last, ROWS, part_width), bf16),
            pltpu.VMEM((PARTS, last, ROWS, part_width), bf16),
            pltpu.VMEM((PARTS, last, ROWS, part_width), bf16),
            dma((2, BLOCKS)),
            dma,
            dma((3, SLOTS)),
            dma((3, SLOTS)),
            dma((len(UNITS),)),
            dma((len(UNITS),)),
            dma((len(UNITS), 4)),
            dma((len(UNITS), 3)),
            dma((len(UNITS),)),
            dma((len(UNITS),)),
        ],
        compiler_params=pltpu.CompilerParams(
            collective_id=0, has_side_effects=True, vmem_limit_bytes=63 * 1024 * 1024
        ),
    )(gate_input.reshape(halved), up_input.reshape(halved), down_weight)


def solution(mesh):
    return jax.shard_map(
        body,
        mesh=mesh,
        in_specs=(P(None, "col", "row"), P(None, "col", "row"), P("row", "col")),
        out_specs=P(None, "row", "col"),
        check_vma=False,
    )
```

```python
import functools

import jax
import jax.numpy as jnp
from jax import lax
from jax.experimental import pallas as pl
from jax.experimental.pallas import tpu as pltpu
from jax.sharding import PartitionSpec as P

MESH = pl.DeviceIdType.MESH

BLOCKS = 8
ROWS = 16
AHEAD = 3
GROUP_SIZES = (8, 6, 6, 6, 6, 5, 6, 4, 6, 3, 3, 2, 3)
LAST = len(GROUP_SIZES) - 1
PARTS = 4

PLUS = (
    [(0, 0, 0), (0, 0, 2), (0, 0, 1), (3, 0, 0), (0, 1, 3), (3, 0, 2), (0, 1, 5), (3, 1, 3), (0, 0, 4), (0, 1, 7)]
    + [(3, 1, 5), (3, 0, 4), (0, 0, 6), (3, 1, 7, 0), (0, 0, 3), (3, 0, 6), (0, 1, 4), (0, 0, 5), (0, 1, 6), (0, 0, 7)]
)
MINUS = (
    [(0, 0, 1), (0, 0, 0), (0, 0, 3), (1, 0, 1), (0, 1, 4), (1, 0, 3), (0, 1, 6), (1, 1, 4), (0, 0, 2), (0, 1, 7)]
    + [(1, 1, 6), (0, 0, 5), (0, 0, 7), (1, 1, 7, 1), (1, 0, 5), (1, 0, 7), (0, 1, 3), (0, 0, 4), (0, 1, 5), (0, 0, 6)]
)
ACROSS = (
    [(0, 0, 3), (0, 0, 4), (0, 0, 5), (0, 0, 6), (0, 0, 7), (3, 0, 0), (1, 0, 1), (2, 0, 0), (2, 0, 1), None]
    + [(1, 0, 0), (2, 0, 2), (3, 0, 2), None, (1, 0, 2), (3, 0, 1), (0, 0, 0), (0, 0, 1), None, (0, 0, 2)]
)
OWN_ORDER = (0, 1, 3, 2, 4, 5, 6, 7)


def plan():
    links = []
    for items, shift_x, shift_y in ((PLUS, 3, 0), (MINUS, 1, 0), (ACROSS, 0, 1)):
        link = []
        for item in items:
            if item is None:
                link.append(None)
                continue
            dx, dy, block = item[:3]
            half = item[3] if len(item) > 3 else None
            link.append(((dx, dy, block), half, ((dx + shift_x) % 4, dy ^ shift_y, block)))
        links.append(link)
    order = [(0, 0, b) for b in range(BLOCKS)]
    arrived_at = {key: -1 for key in order}
    slots = max(len(link) for link in links)
    for slot in range(slots):
        for link in links:
            if slot < len(link) and link[slot]:
                key = link[slot][2]
                if key not in arrived_at:
                    order.append(key)
                arrived_at[key] = slot
    assert len(order) == 8 * BLOCKS
    issue = {}
    for link in links:
        for slot, item in enumerate(link):
            source = item[0] if item else order[0]
            issue.setdefault(max(arrived_at[source], slot - AHEAD, -1), []).append((links.index(link), slot))
    groups, at = [], 0
    for size in GROUP_SIZES:
        groups.append(sorted(order[at : at + size]))
        at += size
    assert at == len(order)
    place = {key: (g, q) for g, group in enumerate(groups) for q, key in enumerate(group)}
    start = [sum(GROUP_SIZES[:g]) for g in range(len(GROUP_SIZES))]
    ready = [max(arrived_at[key] for key in group) for group in groups]
    return links, groups, place, start, ready, slots, issue


LINKS, GROUPS, PLACE, START, READY, SLOTS, ISSUE = plan()
N_GROUPS = len(GROUPS)
UNITS = [(g, 0) for g in range(LAST)] + [(LAST, part) for part in range(PARTS)]
TILE_N = 512


def runs_of(g):
    runs = []
    for dx in range(4):
        places = [q for q, key in enumerate(GROUPS[g]) if key[0] == dx]
        if places:
            rank = sum(key[0] == dx for group in GROUPS[:g] for key in group)
            runs.append((dx, places[0], len(places), rank))
    return runs


def y_runs_of(g, dx):
    runs = []
    for dy in range(2):
        places = [q for q, key in enumerate(GROUPS[g]) if key[:2] == (dx, dy)]
        if places:
            rank = sum(key[:2] == (dx, dy) for group in GROUPS[:g] for key in group)
            runs.append((dy, places[0], len(places), rank))
    return runs


def kernel(gate_ref, up_ref, weight_ref, out_ref, *scratch):
    hidden = scratch[:N_GROUPS]
    (gate_buf, up_buf, weight, result, halves, z_out, z_in, y_out, y_in) = scratch[N_GROUPS : N_GROUPS + 9]
    last_bufs = scratch[N_GROUPS + 9 : N_GROUPS + 15]
    (load_sem, weight_sem, send_sem, recv_sem, pair_send, pair_recv, z_send, z_recv, y_send, y_recv) = scratch[N_GROUPS + 15 :]
    result_last, halves_last, z_out_last, z_in_last, y_out_last, y_in_last = last_bufs
    row = lax.axis_index("row")
    col = lax.axis_index("col")
    y_hi, z, core = row // 8, (row // 2) % 4, row % 2
    y_lo, x = col // 4, col % 4
    across = (row, (1 - y_lo) * 4 + x)
    plus = (row, y_lo * 4 + (x + 1) % 4)
    minus = (row, y_lo * 4 + (x + 3) % 4)
    partner = (y_hi * 8 + z * 2 + (1 - core), col)
    far = ((1 - y_hi) * 8 + z * 2 + core, col)
    targets = (plus, minus, across)
    root_dx = (z + 4 - x) % 4
    final_dy = (y_hi + y_lo) % 2

    def z_device(other):
        return (y_hi * 8 + other * 2 + core, col)

    barrier = pltpu.get_barrier_semaphore()
    for device in (plus, minus, across, partner, far, z_device((z + 1) % 4), z_device((z + 2) % 4), z_device((z + 3) % 4)):
        pl.semaphore_signal(barrier, inc=1, device_id=device, device_id_type=MESH)

    def load(block):
        s, j = divmod(block, 4)
        rows = pl.ds(j * ROWS, ROWS)
        return (
            pltpu.make_async_copy(gate_ref.at[s, :, rows, :], gate_buf.at[block], load_sem.at[0, block]),
            pltpu.make_async_copy(up_ref.at[s, :, rows, :], up_buf.at[block], load_sem.at[1, block]),
        )

    for block in OWN_ORDER:
        for copy in load(block):
            copy.start()
    weight_copy = pltpu.make_async_copy(weight_ref, weight, weight_sem)
    weight_copy.start()

    def view(key, half):
        g, q = PLACE[key]
        return hidden[g].at[q] if half is None else hidden[g].at[q, half]

    def transfer(link, slot):
        source, half, target = LINKS[link][slot]
        return pltpu.make_async_remote_copy(
            src_ref=view(source, half),
            dst_ref=view(target, half),
            send_sem=send_sem.at[link, slot],
            recv_sem=recv_sem.at[link, slot],
            device_id=targets[link],
            device_id_type=MESH,
        )

    pending = sorted((i for i in ISSUE[-1] if LINKS[i[0]][i[1]]), key=lambda i: i[1])
    done = set()
    for block in OWN_ORDER:
        for copy in load(block):
            copy.wait()

        def gate_half(h, carry, block=block):
            gate = gate_buf[block, h].astype(jnp.float32)
            up = up_buf[block, h].astype(jnp.float32)
            hidden[0][block, h] = ((0.5 * gate) * (1.0 + jnp.tanh(0.5 * gate)) * up).astype(jnp.bfloat16)
            return carry

        lax.fori_loop(0, 2, gate_half, 0)
        done.add(block)
        if len(done) < 3:
            continue
        if len(done) == 3:
            pl.semaphore_wait(barrier, 8)
        for link, slot in list(pending):
            if LINKS[link][slot][0][2] in done and not any(l == link and s < slot for l, s in pending):
                transfer(link, slot).start()
                pending.remove((link, slot))
    assert not pending
    weight_copy.wait()
    width = weight.shape[1]

    def sums(g, part):
        return halves_last.at[part] if g == LAST else halves.at[pl.ds(START[g], GROUP_SIZES[g])]

    def outgoing(g, part):
        return z_out_last.at[part] if g == LAST else z_out.at[pl.ds(START[g], GROUP_SIZES[g])]

    def products(g, part, half):
        return result_last.at[part, half] if g == LAST else result.at[g % 2, half, pl.ds(0, GROUP_SIZES[g])]

    def z_landing(g, part, offset, run):
        _, first, count, rank = run
        return z_in_last.at[part, offset, pl.ds(first, count)] if g == LAST else z_in.at[offset, pl.ds(rank, count)]

    def y_leaving(g, part, run, y_run):
        _, z_first, _, rank = run
        _, first, count, _ = y_run
        if g == LAST:
            return y_out_last.at[part, pl.ds(first, count)]
        return y_out.at[pl.ds(rank + first - z_first, count)]

    def y_landing(g, part, y_run):
        _, first, count, rank = y_run
        return y_in_last.at[part, pl.ds(first, count)] if g == LAST else y_in.at[pl.ds(rank, count)]

    def remote(source, target, sent, received, device):
        return pltpu.make_async_remote_copy(
            src_ref=source, dst_ref=target, send_sem=sent, recv_sem=received, device_id=device, device_id_type=MESH
        )

    def pair_copy(g, part):
        unit = g + part
        return remote(products(g, part, 1 - core), sums(g, part), pair_send.at[unit], pair_recv.at[unit], partner)

    def z_copy(g, part, run):
        dx, first, count, _ = run
        root = (x + dx) % 4
        offset = (z + 4 - root) % 4 - 1
        unit = g + part
        source = outgoing(g, part).at[pl.ds(first, count)]
        return root, remote(
            source, z_landing(g, part, offset, run), z_send.at[unit, dx], z_recv.at[unit, offset], z_device(root)
        )

    def z_arrival(g, part, offset, run):
        landed = z_landing(g, part, offset, run)
        return remote(landed, landed, z_send.at[0, 0], z_recv.at[g + part, offset], z_device((z + 1) % 4))

    def y_copy(g, part, run, y_run):
        unit = g + part
        return remote(y_leaving(g, part, run, y_run), y_landing(g, part, y_run), y_send.at[unit], y_recv.at[unit], far)

    def multiply(g, part):
        size = GROUP_SIZES[g]
        span = width // PARTS if g == LAST else width

        def tile(n, carry):
            columns = pl.ds(pl.multiple_of(n * TILE_N, TILE_N), TILE_N)
            taken = pl.ds(pl.multiple_of(n * TILE_N + part * span, TILE_N), TILE_N)
            left = hidden[g][...].reshape(size * 2 * ROWS, -1)
            value = jnp.dot(left, weight[:, taken], preferred_element_type=jnp.float32)
            value = value.reshape(size, 2, ROWS, TILE_N)
            for half in range(2):
                products(g, part, half)[:, :, columns] = value[:, half]
            return carry

        lax.fori_loop(0, span // TILE_N, tile, 0)
        pair_copy(g, part).start()

    def tiles(count, span, body):
        steps = span // TILE_N

        def one(i, carry):
            body(i // steps, pl.ds(pl.multiple_of(i % steps * TILE_N, TILE_N), TILE_N))
            return carry

        lax.fori_loop(0, count * steps, one, 0)

    def add_pair(g, part):
        pair_copy(g, part).wait_recv()
        own, total, out = products(g, part, core), sums(g, part), outgoing(g, part)

        def add(q, columns):
            value = total[q, :, columns] + own[q, :, columns]
            total[q, :, columns] = value
            out[q, :, columns] = value.astype(jnp.bfloat16)

        tiles(GROUP_SIZES[g], total.shape[-1], add)
        for run in runs_of(g):
            root, copy = z_copy(g, part, run)

            @pl.when(root != z)
            def _():
                copy.start()

        pair_copy(g, part).wait_send()

    def add_z(g, part=0):
        for run in runs_of(g):
            dx, first, count, _ = run

            @pl.when(root_dx == dx)
            def _():
                total = sums(g, part)
                for offset in range(3):
                    z_arrival(g, part, offset, run).wait_recv()
                for y_run in y_runs_of(g, dx):
                    dy, y_first, y_count, _ = y_run
                    leaving = y_leaving(g, part, run, y_run)

                    def add(q, columns):
                        value = total[y_first + q, :, columns]
                        for offset in range(3):
                            landed = z_landing(g, part, offset, run)
                            value = value + landed[y_first - first + q, :, columns].astype(jnp.float32)
                        total[y_first + q, :, columns] = value
                        leaving[q, :, columns] = value.astype(jnp.bfloat16)

                    tiles(y_count, total.shape[-1], add)

                    @pl.when(final_dy != dy)
                    def _():
                        y_copy(g, part, run, y_run).start()

    def add_y(g, part=0):
        for run in runs_of(g):
            dx = run[0]
            for y_run in y_runs_of(g, dx):
                dy, y_first, y_count, _ = y_run

                @pl.when((root_dx == dx) & (final_dy == dy))
                def _():
                    total, landed = sums(g, part), y_landing(g, part, y_run)
                    span = total.shape[-1]
                    y_copy(g, part, run, y_run).wait_recv()
                    for q in range(y_count):
                        s, j = divmod(GROUPS[g][y_first + q][2], 4)

                        def add(_, columns):
                            value = total[y_first + q, :, columns] + landed[q, :, columns].astype(jnp.float32)
                            taken = pl.ds(pl.multiple_of(columns.start + part * span, TILE_N), TILE_N)
                            out_ref[s, pl.ds(j * ROWS, ROWS), taken] = value.astype(jnp.bfloat16)

                        tiles(1, span, add)

    z_work = {4: (0, 1), 5: (2,), 6: (3,), 7: (4,), 8: (5,), 9: (6,), 10: (7,), 11: (8,)}
    y_work = {7: (0, 1), 8: (2,), 9: (3,), 10: (4,), 11: (5,)}

    def step(g):
        if g > 9:
            add_pair(g - 1, 0)
        multiply(g, 0)
        for older in z_work.get(g, ()):
            add_z(older)
        for older in y_work.get(g, ()):
            add_y(older)
        if g < 9:
            add_pair(g, 0)

    def last_step():
        add_pair(LAST - 1, 0)
        multiply(LAST, 0)
        for part in range(1, PARTS):
            multiply(LAST, part)
            if part > 1:
                add_pair(LAST, part - 2)
        add_pair(LAST, PARTS - 2)
        add_z(LAST - 3)
        add_pair(LAST, PARTS - 1)
        add_y(LAST - 6)
        add_z(LAST - 2)
        add_y(LAST - 5)
        add_z(LAST - 1)
        add_y(LAST - 4)
        for part in range(PARTS):
            add_z(LAST, part)
        for g in range(LAST - 3, LAST):
            add_y(g)
        for part in range(PARTS):
            add_y(LAST, part)

    step(0)
    for slot in range(SLOTS):
        for link in range(3):
            if LINKS[link][slot]:
                transfer(link, slot).wait_recv()
        for link, later in sorted(ISSUE.get(slot, ()), key=lambda i: i[1]):
            if LINKS[link][later]:
                transfer(link, later).start()
        for g in range(1, N_GROUPS):
            if READY[g] == slot:
                step(g) if g < LAST else last_step()

    for link in range(3):
        for slot in range(SLOTS):
            if LINKS[link][slot]:
                transfer(link, slot).wait_send()
    for g, part in UNITS:
        for run in runs_of(g):
            root, copy = z_copy(g, part, run)

            @pl.when(root != z)
            def _():
                copy.wait_send()

            for y_run in y_runs_of(g, run[0]):

                @pl.when((root_dx == run[0]) & (final_dy != y_run[0]))
                def _():
                    y_copy(g, part, run, y_run).wait_send()


def body(gate_input, up_input, down_weight):
    seqs, tokens, units = gate_input.shape
    width = down_weight.shape[1]
    halved = (seqs, 2, tokens // 2, units)
    bf16, f32 = jnp.bfloat16, jnp.float32
    dma = pltpu.SemaphoreType.DMA
    last, part_width = GROUP_SIZES[LAST], width // PARTS
    earlier = 8 * BLOCKS - last
    any_spec = pl.BlockSpec(memory_space=pl.ANY)
    return pl.pallas_call(
        kernel,
        out_shape=jax.ShapeDtypeStruct((seqs, tokens // 2, width), bf16),
        in_specs=[any_spec, any_spec, any_spec],
        out_specs=pl.BlockSpec(memory_space=pltpu.VMEM),
        scratch_shapes=[
            *[pltpu.VMEM((size, 2, ROWS, units), bf16) for size in GROUP_SIZES],
            pltpu.VMEM((BLOCKS, 2, ROWS, units), bf16),
            pltpu.VMEM((BLOCKS, 2, ROWS, units), bf16),
            pltpu.VMEM((units, width), bf16),
            pltpu.VMEM((2, 2, BLOCKS, ROWS, width), f32),
            pltpu.VMEM((earlier, ROWS, width), f32),
            pltpu.VMEM((earlier, ROWS, width), bf16),
            pltpu.VMEM((3, 2 * BLOCKS, ROWS, width), bf16),
            pltpu.VMEM((2 * BLOCKS, ROWS, width), bf16),
            pltpu.VMEM((BLOCKS, ROWS, width), bf16),
            pltpu.VMEM((PARTS, 2, last, ROWS, part_width), f32),
            pltpu.VMEM((PARTS, last, ROWS, part_width), f32),
            pltpu.VMEM((PARTS, last, ROWS, part_width), bf16),
            pltpu.VMEM((PARTS, 3, last, ROWS, part_width), bf16),
            pltpu.VMEM((PARTS, last, ROWS, part_width), bf16),
            pltpu.VMEM((PARTS, last, ROWS, part_width), bf16),
            dma((2, BLOCKS)),
            dma,
            dma((3, SLOTS)),
            dma((3, SLOTS)),
            dma((len(UNITS),)),
            dma((len(UNITS),)),
            dma((len(UNITS), 4)),
            dma((len(UNITS), 3)),
            dma((len(UNITS),)),
            dma((len(UNITS),)),
        ],
        compiler_params=pltpu.CompilerParams(
            collective_id=0, has_side_effects=True, vmem_limit_bytes=53 * 1024 * 1024
        ),
    )(gate_input.reshape(halved), up_input.reshape(halved), down_weight)


def solution(mesh):
    return jax.shard_map(
        body,
        mesh=mesh,
        in_specs=(P(None, "col", "row"), P(None, "col", "row"), P("row", "col")),
        out_specs=P(None, "row", "col"),
        check_vma=False,
    )
```

```python
import functools

import jax
import jax.numpy as jnp
from jax import lax
from jax.experimental import pallas as pl
from jax.experimental.pallas import tpu as pltpu
from jax.sharding import PartitionSpec as P

MESH = pl.DeviceIdType.MESH

BLOCKS = 8
ROWS = 16
AHEAD = 4
GROUP_SIZES = (8, 6, 6, 6, 6, 5, 6, 4, 6, 3, 3, 2, 3)
LAST = len(GROUP_SIZES) - 1
PARTS = 4

PLUS = (
    [(0, 0, 0), (0, 0, 2), (0, 0, 1), (3, 0, 0), (0, 1, 3), (3, 0, 2), (0, 1, 5), (3, 1, 3), (0, 0, 4), (0, 1, 7)]
    + [(3, 1, 5), (3, 0, 4), (0, 0, 6), (3, 1, 7, 0), (0, 0, 3), (3, 0, 6), (0, 1, 4), (0, 0, 5), (0, 1, 6), (0, 0, 7)]
)
MINUS = (
    [(0, 0, 1), (0, 0, 0), (0, 0, 3), (1, 0, 1), (0, 1, 4), (1, 0, 3), (0, 1, 6), (1, 1, 4), (0, 0, 2), (0, 1, 7)]
    + [(1, 1, 6), (0, 0, 5), (0, 0, 7), (1, 1, 7, 1), (1, 0, 5), (1, 0, 7), (0, 1, 3), (0, 0, 4), (0, 1, 5), (0, 0, 6)]
)
ACROSS = (
    [(0, 0, 3), (0, 0, 4), (0, 0, 5), (0, 0, 6), (0, 0, 7), (3, 0, 0), (1, 0, 1), (2, 0, 0), (2, 0, 1), None]
    + [(1, 0, 0), (2, 0, 2), (3, 0, 2), None, (1, 0, 2), (3, 0, 1), (0, 0, 0), (0, 0, 1), None, (0, 0, 2)]
)
OWN_ORDER = (0, 1, 3, 2, 4, 5, 6, 7)


def plan():
    links = []
    for items, shift_x, shift_y in ((PLUS, 3, 0), (MINUS, 1, 0), (ACROSS, 0, 1)):
        link = []
        for item in items:
            if item is None:
                link.append(None)
                continue
            dx, dy, block = item[:3]
            half = item[3] if len(item) > 3 else None
            link.append(((dx, dy, block), half, ((dx + shift_x) % 4, dy ^ shift_y, block)))
        links.append(link)
    order = [(0, 0, b) for b in range(BLOCKS)]
    arrived_at = {key: -1 for key in order}
    slots = max(len(link) for link in links)
    for slot in range(slots):
        for link in links:
            if slot < len(link) and link[slot]:
                key = link[slot][2]
                if key not in arrived_at:
                    order.append(key)
                arrived_at[key] = slot
    assert len(order) == 8 * BLOCKS
    issue = {}
    for link in links:
        for slot, item in enumerate(link):
            source = item[0] if item else order[0]
            issue.setdefault(max(arrived_at[source], slot - AHEAD, -1), []).append((links.index(link), slot))
    groups, at = [], 0
    for size in GROUP_SIZES:
        groups.append(sorted(order[at : at + size]))
        at += size
    assert at == len(order)
    place = {key: (g, q) for g, group in enumerate(groups) for q, key in enumerate(group)}
    start = [sum(GROUP_SIZES[:g]) for g in range(len(GROUP_SIZES))]
    ready = [max(arrived_at[key] for key in group) for group in groups]
    return links, groups, place, start, ready, slots, issue


LINKS, GROUPS, PLACE, START, READY, SLOTS, ISSUE = plan()
N_GROUPS = len(GROUPS)
UNITS = [(g, 0) for g in range(LAST)] + [(LAST, part) for part in range(PARTS)]
TILE_N = 512


def runs_of(g):
    runs = []
    for dx in range(4):
        places = [q for q, key in enumerate(GROUPS[g]) if key[0] == dx]
        if places:
            rank = sum(key[0] == dx for group in GROUPS[:g] for key in group)
            runs.append((dx, places[0], len(places), rank))
    return runs


def y_runs_of(g, dx):
    runs = []
    for dy in range(2):
        places = [q for q, key in enumerate(GROUPS[g]) if key[:2] == (dx, dy)]
        if places:
            rank = sum(key[:2] == (dx, dy) for group in GROUPS[:g] for key in group)
            runs.append((dy, places[0], len(places), rank))
    return runs


def kernel(gate_ref, up_ref, weight_ref, out_ref, *scratch):
    hidden = scratch[:N_GROUPS]
    (gate_buf, up_buf, weight, result, halves, z_out, z_in, y_out, y_in) = scratch[N_GROUPS : N_GROUPS + 9]
    last_bufs = scratch[N_GROUPS + 9 : N_GROUPS + 15]
    (load_sem, weight_sem, send_sem, recv_sem, pair_send, pair_recv, z_send, z_recv, y_send, y_recv) = scratch[N_GROUPS + 15 :]
    result_last, halves_last, z_out_last, z_in_last, y_out_last, y_in_last = last_bufs
    row = lax.axis_index("row")
    col = lax.axis_index("col")
    y_hi, z, core = row // 8, (row // 2) % 4, row % 2
    y_lo, x = col // 4, col % 4
    across = (row, (1 - y_lo) * 4 + x)
    plus = (row, y_lo * 4 + (x + 1) % 4)
    minus = (row, y_lo * 4 + (x + 3) % 4)
    partner = (y_hi * 8 + z * 2 + (1 - core), col)
    far = ((1 - y_hi) * 8 + z * 2 + core, col)
    targets = (plus, minus, across)
    root_dx = (z + 4 - x) % 4
    final_dy = (y_hi + y_lo) % 2

    def z_device(other):
        return (y_hi * 8 + other * 2 + core, col)

    barrier = pltpu.get_barrier_semaphore()
    for device in (plus, minus, across, partner, far, z_device((z + 1) % 4), z_device((z + 2) % 4), z_device((z + 3) % 4)):
        pl.semaphore_signal(barrier, inc=1, device_id=device, device_id_type=MESH)

    def load(block):
        s, j = divmod(block, 4)
        rows = pl.ds(j * ROWS, ROWS)
        return (
            pltpu.make_async_copy(gate_ref.at[s, :, rows, :], gate_buf.at[block], load_sem.at[0, block]),
            pltpu.make_async_copy(up_ref.at[s, :, rows, :], up_buf.at[block], load_sem.at[1, block]),
        )

    for block in OWN_ORDER:
        for copy in load(block):
            copy.start()
    weight_copy = pltpu.make_async_copy(weight_ref, weight, weight_sem)
    weight_copy.start()

    def view(key, half):
        g, q = PLACE[key]
        return hidden[g].at[q] if half is None else hidden[g].at[q, half]

    def transfer(link, slot):
        source, half, target = LINKS[link][slot]
        return pltpu.make_async_remote_copy(
            src_ref=view(source, half),
            dst_ref=view(target, half),
            send_sem=send_sem.at[link, slot],
            recv_sem=recv_sem.at[link, slot],
            device_id=targets[link],
            device_id_type=MESH,
        )

    pending = sorted((i for i in ISSUE[-1] if LINKS[i[0]][i[1]]), key=lambda i: i[1])
    done = set()
    for block in OWN_ORDER:
        for copy in load(block):
            copy.wait()

        def gate_half(h, carry, block=block):
            gate = gate_buf[block, h].astype(jnp.float32)
            up = up_buf[block, h].astype(jnp.float32)
            hidden[0][block, h] = ((0.5 * gate) * (1.0 + jnp.tanh(0.5 * gate)) * up).astype(jnp.bfloat16)
            return carry

        lax.fori_loop(0, 2, gate_half, 0)
        done.add(block)
        if len(done) < 3:
            continue
        if len(done) == 3:
            pl.semaphore_wait(barrier, 8)
        for link, slot in list(pending):
            if LINKS[link][slot][0][2] in done and not any(l == link and s < slot for l, s in pending):
                transfer(link, slot).start()
                pending.remove((link, slot))
    assert not pending
    weight_copy.wait()
    width = weight.shape[1]

    def sums(g, part):
        return halves_last.at[part] if g == LAST else halves.at[pl.ds(START[g], GROUP_SIZES[g])]

    def outgoing(g, part):
        return z_out_last.at[part] if g == LAST else z_out.at[pl.ds(START[g], GROUP_SIZES[g])]

    def products(g, part, half):
        return result_last.at[part, half] if g == LAST else result.at[g % 2, half, pl.ds(0, GROUP_SIZES[g])]

    def z_landing(g, part, offset, run):
        _, first, count, rank = run
        return z_in_last.at[part, offset, pl.ds(first, count)] if g == LAST else z_in.at[offset, pl.ds(rank, count)]

    def y_leaving(g, part, run, y_run):
        _, z_first, _, rank = run
        _, first, count, _ = y_run
        if g == LAST:
            return y_out_last.at[part, pl.ds(first, count)]
        return y_out.at[pl.ds(rank + first - z_first, count)]

    def y_landing(g, part, y_run):
        _, first, count, rank = y_run
        return y_in_last.at[part, pl.ds(first, count)] if g == LAST else y_in.at[pl.ds(rank, count)]

    def remote(source, target, sent, received, device):
        return pltpu.make_async_remote_copy(
            src_ref=source, dst_ref=target, send_sem=sent, recv_sem=received, device_id=device, device_id_type=MESH
        )

    def pair_copy(g, part):
        unit = g + part
        return remote(products(g, part, 1 - core), sums(g, part), pair_send.at[unit], pair_recv.at[unit], partner)

    def z_copy(g, part, run):
        dx, first, count, _ = run
        root = (x + dx) % 4
        offset = (z + 4 - root) % 4 - 1
        unit = g + part
        source = outgoing(g, part).at[pl.ds(first, count)]
        return root, remote(
            source, z_landing(g, part, offset, run), z_send.at[unit, dx], z_recv.at[unit, offset], z_device(root)
        )

    def z_arrival(g, part, offset, run):
        landed = z_landing(g, part, offset, run)
        return remote(landed, landed, z_send.at[0, 0], z_recv.at[g + part, offset], z_device((z + 1) % 4))

    def y_copy(g, part, run, y_run):
        unit = g + part
        return remote(y_leaving(g, part, run, y_run), y_landing(g, part, y_run), y_send.at[unit], y_recv.at[unit], far)

    def multiply(g, part):
        size = GROUP_SIZES[g]
        span = width // PARTS if g == LAST else width

        step_n = min(1024, span)

        def tile(n, carry):
            columns = pl.ds(pl.multiple_of(n * step_n, step_n), step_n)
            taken = pl.ds(pl.multiple_of(n * step_n + part * span, step_n), step_n)
            left = hidden[g][...].reshape(size * 2 * ROWS, -1)
            value = jnp.dot(left, weight[:, taken], preferred_element_type=jnp.float32)
            value = value.reshape(size, 2, ROWS, step_n)
            for half in range(2):
                products(g, part, half)[:, :, columns] = value[:, half]
            return carry

        lax.fori_loop(0, span // step_n, tile, 0)
        pair_copy(g, part).start()

    def tiles(count, span, body):
        steps = span // TILE_N

        def one(i, carry):
            body(i // steps, pl.ds(pl.multiple_of(i % steps * TILE_N, TILE_N), TILE_N))
            return carry

        lax.fori_loop(0, count * steps, one, 0)

    def add_pair(g, part):
        pair_copy(g, part).wait_recv()
        own, total, out = products(g, part, core), sums(g, part), outgoing(g, part)

        def add(q, columns):
            value = total[q, :, columns] + own[q, :, columns]
            total[q, :, columns] = value
            out[q, :, columns] = value.astype(jnp.bfloat16)

        tiles(GROUP_SIZES[g], total.shape[-1], add)
        for run in runs_of(g):
            root, copy = z_copy(g, part, run)

            @pl.when(root != z)
            def _():
                copy.start()

        pair_copy(g, part).wait_send()

    def add_z(g, part=0):
        for run in runs_of(g):
            dx, first, count, _ = run

            @pl.when(root_dx == dx)
            def _():
                total = sums(g, part)
                for offset in range(3):
                    z_arrival(g, part, offset, run).wait_recv()
                for y_run in y_runs_of(g, dx):
                    dy, y_first, y_count, _ = y_run
                    leaving = y_leaving(g, part, run, y_run)

                    def add(q, columns):
                        value = total[y_first + q, :, columns]
                        for offset in range(3):
                            landed = z_landing(g, part, offset, run)
                            value = value + landed[y_first - first + q, :, columns].astype(jnp.float32)
                        total[y_first + q, :, columns] = value
                        leaving[q, :, columns] = value.astype(jnp.bfloat16)

                    tiles(y_count, total.shape[-1], add)

                    @pl.when(final_dy != dy)
                    def _():
                        y_copy(g, part, run, y_run).start()

    def add_y(g, part=0):
        for run in runs_of(g):
            dx = run[0]
            for y_run in y_runs_of(g, dx):
                dy, y_first, y_count, _ = y_run

                @pl.when((root_dx == dx) & (final_dy == dy))
                def _():
                    total, landed = sums(g, part), y_landing(g, part, y_run)
                    span = total.shape[-1]
                    y_copy(g, part, run, y_run).wait_recv()
                    for q in range(y_count):
                        s, j = divmod(GROUPS[g][y_first + q][2], 4)

                        def add(_, columns):
                            value = total[y_first + q, :, columns] + landed[q, :, columns].astype(jnp.float32)
                            taken = pl.ds(pl.multiple_of(columns.start + part * span, TILE_N), TILE_N)
                            out_ref[s, pl.ds(j * ROWS, ROWS), taken] = value.astype(jnp.bfloat16)

                        tiles(1, span, add)

    z_work = {4: (0, 1), 5: (2,), 6: (3,), 7: (4,), 8: (5,), 9: (6,), 10: (7,), 11: (8,)}
    y_work = {7: (0, 1), 8: (2,), 9: (3,), 10: (4,), 11: (5,)}

    def step(g):
        if g > 9:
            add_pair(g - 1, 0)
        multiply(g, 0)
        for older in z_work.get(g, ()):
            add_z(older)
        for older in y_work.get(g, ()):
            add_y(older)
        if g < 9:
            add_pair(g, 0)

    def last_step():
        add_pair(LAST - 1, 0)
        multiply(LAST, 0)
        for part in range(1, PARTS):
            multiply(LAST, part)
            if part > 1:
                add_pair(LAST, part - 2)
        add_pair(LAST, PARTS - 2)
        add_z(LAST - 3)
        add_pair(LAST, PARTS - 1)
        add_y(LAST - 6)
        add_z(LAST - 2)
        add_y(LAST - 5)
        add_z(LAST - 1)
        add_y(LAST - 4)
        for part in range(PARTS):
            add_z(LAST, part)
        for g in range(LAST - 3, LAST):
            add_y(g)
        for part in range(PARTS):
            add_y(LAST, part)

    step(0)
    for slot in range(SLOTS):
        for link in range(3):
            if LINKS[link][slot]:
                transfer(link, slot).wait_recv()
        for link, later in sorted(ISSUE.get(slot, ()), key=lambda i: i[1]):
            if LINKS[link][later]:
                transfer(link, later).start()
        for g in range(1, N_GROUPS):
            if READY[g] == slot:
                step(g) if g < LAST else last_step()

    for link in range(3):
        for slot in range(SLOTS):
            if LINKS[link][slot]:
                transfer(link, slot).wait_send()
    for g, part in UNITS:
        for run in runs_of(g):
            root, copy = z_copy(g, part, run)

            @pl.when(root != z)
            def _():
                copy.wait_send()

            for y_run in y_runs_of(g, run[0]):

                @pl.when((root_dx == run[0]) & (final_dy != y_run[0]))
                def _():
                    y_copy(g, part, run, y_run).wait_send()


def body(gate_input, up_input, down_weight):
    seqs, tokens, units = gate_input.shape
    width = down_weight.shape[1]
    halved = (seqs, 2, tokens // 2, units)
    bf16, f32 = jnp.bfloat16, jnp.float32
    dma = pltpu.SemaphoreType.DMA
    last, part_width = GROUP_SIZES[LAST], width // PARTS
    earlier = 8 * BLOCKS - last
    any_spec = pl.BlockSpec(memory_space=pl.ANY)
    return pl.pallas_call(
        kernel,
        out_shape=jax.ShapeDtypeStruct((seqs, tokens // 2, width), bf16),
        in_specs=[any_spec, any_spec, any_spec],
        out_specs=pl.BlockSpec(memory_space=pltpu.VMEM),
        scratch_shapes=[
            *[pltpu.VMEM((size, 2, ROWS, units), bf16) for size in GROUP_SIZES],
            pltpu.VMEM((BLOCKS, 2, ROWS, units), bf16),
            pltpu.VMEM((BLOCKS, 2, ROWS, units), bf16),
            pltpu.VMEM((units, width), bf16),
            pltpu.VMEM((2, 2, BLOCKS, ROWS, width), f32),
            pltpu.VMEM((earlier, ROWS, width), f32),
            pltpu.VMEM((earlier, ROWS, width), bf16),
            pltpu.VMEM((3, 2 * BLOCKS, ROWS, width), bf16),
            pltpu.VMEM((2 * BLOCKS, ROWS, width), bf16),
            pltpu.VMEM((BLOCKS, ROWS, width), bf16),
            pltpu.VMEM((PARTS, 2, last, ROWS, part_width), f32),
            pltpu.VMEM((PARTS, last, ROWS, part_width), f32),
            pltpu.VMEM((PARTS, last, ROWS, part_width), bf16),
            pltpu.VMEM((PARTS, 3, last, ROWS, part_width), bf16),
            pltpu.VMEM((PARTS, last, ROWS, part_width), bf16),
            pltpu.VMEM((PARTS, last, ROWS, part_width), bf16),
            dma((2, BLOCKS)),
            dma,
            dma((3, SLOTS)),
            dma((3, SLOTS)),
            dma((len(UNITS),)),
            dma((len(UNITS),)),
            dma((len(UNITS), 4)),
            dma((len(UNITS), 3)),
            dma((len(UNITS),)),
            dma((len(UNITS),)),
        ],
        compiler_params=pltpu.CompilerParams(
            collective_id=0, has_side_effects=True, vmem_limit_bytes=53 * 1024 * 1024
        ),
    )(gate_input.reshape(halved), up_input.reshape(halved), down_weight)


def solution(mesh):
    return jax.shard_map(
        body,
        mesh=mesh,
        in_specs=(P(None, "col", "row"), P(None, "col", "row"), P("row", "col")),
        out_specs=P(None, "row", "col"),
        check_vma=False,
    )
```
